512 devices in a mesh: section: 8 (over x, core), expert: 64 (over y, z).
Axes of the slice: x: 4, y: 4, z: 16, core: 2. Of those that a mesh axis runs over, the one named last changes fastest.
Arguments:
- images: bfloat16 [512, 256, 1408], P(('section', 'expert')), may hold values from -6 to 6
- norm_gain: bfloat16 [1408], replicated, may hold values from 0.5 to 1.5
- slot_map: bfloat16 [1408, 64], replicated, may hold values from -0.15625 to 0.15625
- logit_scale: float32 [1], replicated, may hold values from 30 to 80
- up_weight: bfloat16 [64, 5120, 1408], P('expert', 'section'), may hold values from -0.625 to 0.625
- down_weight: bfloat16 [64, 5120, 1408], P('expert', 'section'), may hold values from -0.3125 to 0.3125
Outputs:
- block_out: bfloat16 [512, 256, 1408], P(('section', 'expert'))
The draws below stay inside these ranges and needn't reach their ends.
All inputs are finite; a program needn't handle non-finite values.
Results may differ from the reference program's by a relative error of at most 0.011.
Values may be sent and summed in bfloat16 or wider, within the bound.
A program may use at most 64 MiB of HBM per device.

```python
import math
import jax
import jax.numpy as jnp
from jax import lax

D = 1408
FF = 5120
TOK = 256
EXPERTS = 64
IMAGES = 512


def levels(rng, extent, shards, low, top_value):
    def one(axis_at, shards_of):
        heights = jax.random.uniform(jax.random.fold_in(jax.random.fold_in(rng, 6), axis_at), (shards_of,), jnp.float32, low / len(shards), top_value / len(shards))
        return jnp.repeat(jnp.exp(heights), extent[axis_at] // shards_of).reshape((-1,) + (1,) * (len(extent) - axis_at - 1))

    loudness = one(*shards[0])
    for cut in shards[1:]:
        loudness = loudness * one(*cut)
    return loudness


def centred(own_key, extent, deviation, reach, split=(), kind=jnp.bfloat16):
    level = levels(own_key, extent, split, -0.22, 0.18) if split else 1.0
    result = jax.random.normal(own_key, extent, jnp.float32) * deviation * level
    return jnp.minimum(jnp.maximum(result, -reach), reach).astype(kind)


def setup_inputs(seed: int = 0) -> dict:
    key_list = jax.random.split(jax.random.key(seed), 7)
    images = centred(key_list[0], (IMAGES, TOK, D), 1.0, 6.0, ((0, 512),))
    norm_gain = jnp.clip(1.0 + 0.1 * jax.random.normal(key_list[1], (D,), jnp.float32), 0.5, 1.5).astype(jnp.bfloat16)
    slot_map = centred(key_list[2], (D, EXPERTS), D ** -0.5, 0.15625)
    logit_scale = jnp.clip(jnp.exp(jax.random.uniform(key_list[3], (1,), jnp.float32, math.log(30.0), math.log(80.0))), 30.0, 80.0)
    up_weight = centred(key_list[4], (EXPERTS, FF, D), (4.0 / D ** 0.5), 0.625, ((0, 64), (1, 8)))
    down_weight = centred(key_list[5], (EXPERTS, FF, D), (4.0 / FF ** 0.5), 0.3125, ((0, 64), (1, 8)))
    return dict(images=images, norm_gain=norm_gain, slot_map=slot_map, logit_scale=logit_scale, up_weight=up_weight, down_weight=down_weight)


epsilon = 1e-06

def normalize(inputs, gain_row):
    values = inputs.astype(jnp.float32)
    spread = lax.optimization_barrier(jnp.mean(values * values, axis=-1, keepdims=True))
    return (values * lax.rsqrt(spread + epsilon) * gain_row.astype(jnp.float32)).astype(jnp.bfloat16)

def weights_from(raw, normed, slot_cols, scale_now):
    values = normed.astype(jnp.float32)
    token_norm = jnp.sqrt(lax.optimization_barrier(jnp.sum(values * values, axis=-1)) + epsilon)
    columns = slot_cols.astype(jnp.float32)
    column_norm = jnp.sqrt(lax.optimization_barrier(jnp.sum(columns * columns, axis=0)) + epsilon)
    logits = scale_now * raw / (token_norm[:, None, :] * column_norm[None, :, None])
    scores = jnp.exp(logits)
    dispatch = (scores / lax.optimization_barrier(jnp.sum(scores, axis=-1, keepdims=True))).astype(jnp.bfloat16)
    combine = (scores / lax.optimization_barrier(jnp.sum(scores, axis=1, keepdims=True))).astype(jnp.bfloat16)
    return (dispatch, combine)

def reference(images, norm_gain, slot_map, logit_scale, up_weight, down_weight):
    normed = normalize(images, norm_gain)
    raw = jnp.einsum('itd,de->iet', normed.astype(jnp.float32), slot_map.astype(jnp.float32))
    dispatch, combine = weights_from(raw, normed, slot_map, logit_scale[0])
    slot_in = jnp.einsum('iet,itd->eid', dispatch.astype(jnp.float32), normed.astype(jnp.float32)).astype(jnp.bfloat16)
    hidden = jax.nn.gelu(jnp.einsum('eid,efd->eif', slot_in.astype(jnp.float32), up_weight.astype(jnp.float32))).astype(jnp.bfloat16)
    slot_out = jnp.einsum('eif,efd->eid', hidden.astype(jnp.float32), down_weight.astype(jnp.float32)).astype(jnp.bfloat16)
    mixed = jnp.einsum('iet,eid->itd', combine.astype(jnp.float32), slot_out.astype(jnp.float32))
    return (images.astype(jnp.float32) + mixed).astype(jnp.bfloat16)
```

```python
import functools

import jax
import jax.numpy as jnp
from jax import lax
from jax.experimental import pallas as pl
from jax.experimental.pallas import tpu as pltpu
from jax.sharding import PartitionSpec as P

epsilon = 1e-06
D = 1408
TOK = 256
E = 64
FH = 640
ROWS = 64
HALF = 32
COLS = D // 128
SLAB = 12
YS, ZS = 4, 16
F32, BF16 = jnp.float32, jnp.bfloat16
MESH = pl.DeviceIdType.MESH
OWN, LEFT, RIGHT, FAR = 0, 1, 2, 3


def to_slabs(value, wide, slabs):
    flat = wide.reshape(ROWS * 16, 128)
    for j in range(COLS):
        flat[pl.ds(j, ROWS, stride=16), :] = value[:, j * 128 : (j + 1) * 128]
    slabs[...] = wide[...][:, :SLAB, :].astype(BF16)


def from_slabs(slabs, wide, out):
    wide[:, :SLAB, :] = slabs[...].astype(F32)
    flat = wide.reshape(ROWS * 16, 128)
    for j in range(COLS):
        out[:, j * 128 : (j + 1) * 128] = flat[pl.ds(j, ROWS, stride=16), :].astype(BF16)


def far_first(i, y, z):
    m = i // 4
    odd = m % 2
    dz = (1 - 2 * odd) * (m // 2 - 8) - odd
    dy = 3 - i % 4
    return ((y + dy) % YS) * ZS + (z + dz + ZS) % ZS


def kernel(
    images, gain, slots, scale, up, down,
    back, comb,
    x_v, gain_v, slots_v, up_v, down_v, up_t, normed, wide,
    send_a, recv_a, send_d, recv_d,
    gat, hid, q_acc, p_out, p_in, q_out, r_far, r_fin,
    load_sem, a2a_sem, bs, br, cs, cr,
):
    sec, me = lax.axis_index("section"), lax.axis_index("expert")
    xs, core = sec // 2, sec % 2
    y, z = me // ZS, me % ZS
    partner = sec + 1 - 2 * core
    right = ((xs + 1) % 4) * 2 + core
    left = ((xs + 3) % 4) * 2 + core

    barrier = pltpu.get_barrier_semaphore()

    def greet(i, c):
        pl.semaphore_signal(barrier, inc=1, device_id={"expert": far_first(i, y, z)}, device_id_type=MESH)
        return c

    lax.fori_loop(0, E - 1, greet, 0)
    for peer in (left, right, partner):
        pl.semaphore_signal(barrier, inc=1, device_id={"section": peer}, device_id_type=MESH)

    loads = [
        pltpu.make_async_copy(src, dst, load_sem.at[i])
        for i, (src, dst) in enumerate(
            ((images.at[0], x_v), (gain, gain_v), (slots, slots_v), (up.at[0], up_v), (down.at[0], down_v))
        )
    ]
    for c in loads:
        c.start()
    for c in loads[:3]:
        c.wait()

    x = x_v[...].astype(F32)
    spread = jnp.mean(x * x, axis=-1, keepdims=True)
    normed[...] = (x * lax.rsqrt(spread + epsilon) * gain_v[...].astype(F32)).astype(BF16)
    n32 = normed[...].astype(F32)
    token_norm = jnp.sqrt(jnp.sum(n32 * n32, axis=-1, keepdims=True) + epsilon)
    cols = slots_v[...].astype(F32)
    column_norm = jnp.sqrt(jnp.sum(cols * cols, axis=0, keepdims=True) + epsilon)
    raw = jnp.dot(normed[...], slots_v[...], preferred_element_type=F32)
    scores = jnp.exp(scale[0] * raw / (token_norm * column_norm))
    dispatch = (scores / jnp.sum(scores, axis=0, keepdims=True)).astype(BF16)
    comb[...] = (scores / jnp.sum(scores, axis=1, keepdims=True)).astype(BF16)
    slot_in = lax.dot_general(dispatch, normed[...], (((0,), (0,)), ((), ())), preferred_element_type=F32)
    to_slabs(slot_in, wide, send_a)

    pl.semaphore_wait(barrier, E - 1 + 3)

    def scatter(src, dst, s, r):
        def one(i, c):
            there = far_first(i, y, z)
            pltpu.make_async_remote_copy(
                src.at[there], dst.at[me], a2a_sem.at[s], a2a_sem.at[r], device_id={"expert": there}, device_id_type=MESH
            ).start()
            return c

        lax.fori_loop(0, E - 1, one, 0)
        dst[me] = src[me]

    def all_but_one(buf, s):
        pltpu.make_async_copy(buf.at[pl.ds(0, E - 1)], buf.at[pl.ds(0, E - 1)], a2a_sem.at[s]).wait()

    scatter(send_a, recv_a, 0, 1)
    for c in loads[3:]:
        c.wait()
    for i in range(FH // 128):
        up_t[:, i * 128 : (i + 1) * 128] = up_v[i * 128 : (i + 1) * 128, :].T
    all_but_one(recv_a, 1)
    from_slabs(recv_a, wide, gat.at[OWN, pl.ds(0, ROWS)])

    def rows(group, half, other=0):
        return gat.at[group, pl.ds(other * ROWS + half * HALF, HALF)]

    def section_copy(src, dst, s, r, i, peer):
        return pltpu.make_async_remote_copy(src, dst, s.at[i], r.at[i], device_id={"section": peer}, device_id_type=MESH)

    hops = [
        section_copy(rows(OWN, 0), rows(LEFT, 0), bs, br, 0, right),
        section_copy(rows(OWN, 1), rows(RIGHT, 1), bs, br, 1, left),
        section_copy(rows(OWN, 1), rows(LEFT, 1), bs, br, 2, right),
        section_copy(rows(OWN, 0), rows(RIGHT, 0), bs, br, 3, left),
        section_copy(gat.at[OWN, pl.ds(0, ROWS)], gat.at[OWN, pl.ds(ROWS, ROWS)], bs, br, 4, partner),
        section_copy(rows(LEFT, 0), rows(FAR, 0), bs, br, 5, right),
        section_copy(rows(RIGHT, 1), rows(FAR, 1), bs, br, 6, left),
    ]
    across = {
        (g, h): section_copy(rows(g, h), rows(g, h, 1), bs, br, 5 + 2 * g + h, partner) for g in (1, 2, 3) for h in (0, 1)
    }

    def mlp(group):
        up_out = jnp.dot(gat[group], up_t[...], preferred_element_type=F32)
        hid[...] = jax.nn.gelu(up_out).astype(BF16)
        part = jnp.dot(hid[...], down_v[...], preferred_element_type=F32)
        q_acc[group] = part[:ROWS]
        p_out[group] = part[ROWS:].astype(BF16)

    pair = [section_copy(p_out.at[g], p_in.at[g], cs, cr, g, partner) for g in range(4)]

    def half(ref, h):
        return ref.at[pl.ds(h * HALF, HALF)]

    sums = [
        section_copy(half(q_out.at[FAR], 0), half(r_far, 0), cs, cr, 4, right),
        section_copy(half(q_out.at[FAR], 1), half(r_far, 1), cs, cr, 5, left),
        section_copy(half(q_out.at[RIGHT], 1), half(r_fin.at[0], 1), cs, cr, 6, right),
        section_copy(half(q_out.at[LEFT], 0), half(r_fin.at[1], 0), cs, cr, 7, left),
        section_copy(half(q_out.at[RIGHT], 0), half(r_fin.at[0], 0), cs, cr, 8, right),
        section_copy(half(q_out.at[LEFT], 1), half(r_fin.at[1], 1), cs, cr, 9, left),
    ]

    def chip_sum(group):
        pair[group].wait_recv()
        q_acc[group] = q_acc[group] + p_in[group].astype(F32)

    for c in hops[:5]:
        c.start()
    hops[4].wait_recv()
    mlp(OWN)
    pair[OWN].start()
    hops[0].wait_recv()
    hops[5].start()
    across[LEFT, 0].start()
    hops[1].wait_recv()
    hops[6].start()
    across[RIGHT, 1].start()
    hops[2].wait_recv()
    across[LEFT, 1].start()
    hops[3].wait_recv()
    across[RIGHT, 0].start()
    chip_sum(OWN)
    for h in (0, 1):
        across[LEFT, h].wait_recv()
    mlp(LEFT)
    pair[LEFT].start()
    for h in (0, 1):
        across[RIGHT, h].wait_recv()
    mlp(RIGHT)
    pair[RIGHT].start()
    for h in (0, 1):
        hops[5 + h].wait_recv()
        across[FAR, h].start()
    chip_sum(LEFT)
    q_out[LEFT, pl.ds(0, HALF)] = q_acc[LEFT, pl.ds(0, HALF)].astype(BF16)
    sums[3].start()
    chip_sum(RIGHT)
    q_out[RIGHT, pl.ds(HALF, HALF)] = q_acc[RIGHT, pl.ds(HALF, HALF)].astype(BF16)
    sums[2].start()
    for h in (0, 1):
        across[FAR, h].wait_recv()
    mlp(FAR)
    pair[FAR].start()
    chip_sum(FAR)
    q_out[FAR] = q_acc[FAR].astype(BF16)
    sums[0].start()
    sums[1].start()
    sums[0].wait_recv()
    q_out[RIGHT, pl.ds(0, HALF)] = (q_acc[RIGHT, pl.ds(0, HALF)] + r_far[pl.ds(0, HALF)].astype(F32)).astype(BF16)
    sums[4].start()
    sums[1].wait_recv()
    q_out[LEFT, pl.ds(HALF, HALF)] = (q_acc[LEFT, pl.ds(HALF, HALF)] + r_far[pl.ds(HALF, HALF)].astype(F32)).astype(BF16)
    sums[5].start()
    for i in (2, 3, 4, 5):
        sums[i].wait_recv()
    result = q_acc[OWN] + r_fin[0].astype(F32) + r_fin[1].astype(F32)
    to_slabs(result, wide, send_d)

    scatter(send_d, recv_d, 2, 3)
    for c in hops + list(across.values()) + pair + sums:
        c.wait_send()
    all_but_one(send_a, 0)
    all_but_one(send_d, 2)
    all_but_one(recv_d, 3)
    from_slabs(recv_d, wide, back)


def exchange(images, norm_gain, slot_map, logit_scale, up_weight, down_weight):
    any_, vmem = pl.BlockSpec(memory_space=pl.ANY), pl.BlockSpec(memory_space=pltpu.VMEM)
    dma = pltpu.SemaphoreType.DMA
    return pl.pallas_call(
        kernel,
        out_shape=(jax.ShapeDtypeStruct((E, D), BF16), jax.ShapeDtypeStruct((TOK, E), BF16)),
        in_specs=[any_, any_, any_, pl.BlockSpec(memory_space=pltpu.SMEM), any_, any_],
        out_specs=(vmem, vmem),
        scratch_shapes=[
            pltpu.VMEM((TOK, D), BF16), pltpu.VMEM((1, D), BF16), pltpu.VMEM((D, E), BF16),
            pltpu.VMEM((FH, D), BF16), pltpu.VMEM((FH, D), BF16), pltpu.VMEM((D, FH), BF16),
            pltpu.VMEM((TOK, D), BF16), pltpu.VMEM((ROWS, 16, 128), F32),
            *[pltpu.VMEM((E, SLAB, 128), BF16)] * 4,
            pltpu.VMEM((4, 2 * ROWS, D), BF16), pltpu.VMEM((2 * ROWS, FH), BF16), pltpu.VMEM((4, ROWS, D), F32),
            pltpu.VMEM((4, ROWS, D), BF16), pltpu.VMEM((4, ROWS, D), BF16), pltpu.VMEM((4, ROWS, D), BF16),
            pltpu.VMEM((ROWS, D), BF16), pltpu.VMEM((2, ROWS, D), BF16),
            dma((5,)), dma((4,)), dma((13,)), dma((13,)), dma((10,)), dma((10,)),
        ],
        compiler_params=pltpu.CompilerParams(collective_id=0, has_side_effects=True, vmem_limit_bytes=56 * 1024 * 1024),
    )(images, norm_gain.reshape(1, D), slot_map, logit_scale, up_weight, down_weight)


def local(images, norm_gain, slot_map, logit_scale, up_weight, down_weight):
    back, comb = exchange(images, norm_gain, slot_map, logit_scale, up_weight, down_weight)
    mixed = jnp.einsum("te,ed->td", comb, back, preferred_element_type=F32)
    return (images.astype(F32) + mixed[None]).astype(BF16)


def solution(mesh):
    return jax.shard_map(
        local,
        mesh=mesh,
        in_specs=(
            P(("section", "expert"), None, None),
            P(),
            P(),
            P(),
            P("expert", "section", None),
            P("expert", "section", None),
        ),
        out_specs=P(("section", "expert"), None, None),
        check_vma=False,
    )
```

```python
import jax
import jax.numpy as jnp
from jax import lax
from jax.experimental import pallas as pl
from jax.experimental.pallas import tpu as pltpu
from jax.sharding import PartitionSpec as P

epsilon = 1e-06
D = 1408
TOK = 256
E = 64
FH = 640
CH = 4
R = 16
COLS = D // 128
SLAB = 12
F32, BF16 = jnp.float32, jnp.bfloat16
MESH = pl.DeviceIdType.MESH
OWN, LEFT, RIGHT, FAR = 0, 1, 2, 3


def to_slabs(value, wide, slabs, n):
    flat = wide.reshape(n * 16, 128)
    for j in range(COLS):
        flat[pl.ds(j, n, stride=16), :] = value[:, j * 128 : (j + 1) * 128]
    slabs[...] = wide[...][:, :SLAB, :].astype(BF16)


def from_slabs(slabs, wide, out, n):
    wide[:, :SLAB, :] = slabs[...].astype(F32)
    flat = wide.reshape(n * 16, 128)
    for j in range(COLS):
        out[:, j * 128 : (j + 1) * 128] = flat[pl.ds(j, n, stride=16), :].astype(BF16)


def kernel(
    images, gain, slots, scale, up, down,
    back, comb,
    x_v, gain_v, slots_v, up_v, down_v, up_t, normed, wide, wide_in, wide_out,
    send_a, recv_a, send_d, recv_d,
    gat, hid, q_acc, p_out, p_in, q_out, r_far, r_fin,
    load_sem, a2a_s, a_r, d_r, bs, br, cs, cr,
):
    sec, me = lax.axis_index("section"), lax.axis_index("expert")
    xs, core = sec // 2, sec % 2
    y, z = me // 16, me % 16
    partner = sec + 1 - 2 * core
    right = ((xs + 1) % 4) * 2 + core
    left = ((xs + 3) % 4) * 2 + core
    by_dy = [((y + dy) % 4) * 16 for dy in (3, 2, 1, 0)]
    by_minus_dy = [((y + 4 - dy) % 4) * 16 for dy in (3, 2, 1, 0)]

    def dz_of(m):
        odd = m % 2
        return (1 - 2 * odd) * (m // 2 - 8) - odd + 16

    loads = [
        pltpu.make_async_copy(src, dst, load_sem.at[i])
        for i, (src, dst) in enumerate(
            ((slots, slots_v), (gain, gain_v), (images.at[0], x_v), (up.at[0], up_v), (down.at[0], down_v))
        )
    ]
    for c in loads:
        c.start()

    barrier = pltpu.get_barrier_semaphore()

    def greet(e):
        pl.semaphore_signal(barrier, inc=1, device_id={"expert": e}, device_id_type=MESH)

    def greet4(m, c):
        there = (z + dz_of(m)) % 16
        for base in by_dy:
            greet(base + there)
        return c

    lax.fori_loop(0, 15, greet4, 0)
    for base in by_dy[:3]:
        greet(base + z)
    for peer in (left, right, partner):
        pl.semaphore_signal(barrier, inc=1, device_id={"section": peer}, device_id_type=MESH)

    for c in loads[:3]:
        c.wait()
    x = x_v[...].astype(F32)
    spread = jnp.mean(x * x, axis=-1, keepdims=True)
    normed[...] = (x * lax.rsqrt(spread + epsilon) * gain_v[...].astype(F32).reshape(1, D)).astype(BF16)
    n32 = normed[...].astype(F32)
    token_norm = jnp.sqrt(jnp.sum(n32 * n32, axis=-1, keepdims=True) + epsilon)
    slot_cols = slots_v[...].T
    cols = slot_cols.astype(F32)
    column_norm = jnp.sqrt(jnp.sum(cols * cols, axis=0, keepdims=True) + epsilon)
    raw = jnp.dot(normed[...], slot_cols, preferred_element_type=F32)
    scores = jnp.exp(scale[0] * raw / (token_norm * column_norm))
    dispatch = (scores / jnp.sum(scores, axis=0, keepdims=True)).astype(BF16)
    comb[...] = (scores / jnp.sum(scores, axis=1, keepdims=True)).astype(BF16)
    slot_in = lax.dot_general(dispatch, normed[...], (((0,), (0,)), ((), ())), preferred_element_type=F32)
    to_slabs(slot_in, wide, send_a, E)

    pl.semaphore_wait(barrier, E - 1 + 3)

    def send_row(chunk, m, k, base, there):
        e = base + there
        i = m * 4 + k
        pltpu.make_async_remote_copy(
            send_a.at[e], recv_a.at[i], a2a_s.at[0], a_r.at[chunk], device_id={"expert": e}, device_id_type=MESH
        ).start()

    for chunk in range(CH):

        def send4(m, c, chunk=chunk):
            there = (z + dz_of(m)) % 16
            for k, base in enumerate(by_dy):
                send_row(chunk, m, k, base, there)
            return c

        lax.fori_loop(4 * chunk, min(4 * chunk + 4, 15), send4, 0)
    for k in range(3):
        send_row(CH - 1, 15, k, by_dy[k], z)
    recv_a[E - 1] = send_a[me]
    for c in loads[3:]:
        c.wait()
    for i in range(FH // 128):
        up_t[:, i * 128 : (i + 1) * 128] = up_v[i * 128 : (i + 1) * 128, :].T

    def slabs_in(buf, n, sem):
        pltpu.make_async_copy(buf.at[pl.ds(0, n)], buf.at[pl.ds(0, n)], sem).wait()

    def section_copy(src, dst, s, r, peer):
        return pltpu.make_async_remote_copy(src, dst, s, r, device_id={"section": peer}, device_id_type=MESH)

    def rows(k, group, n=1, other=0):
        return gat.at[k, pl.ds(64 * other + R * group, R * n)]

    def b_copy(k, i, src, dst, peer):
        return section_copy(src, dst, bs.at[k, i], br.at[k, i], peer)

    def c_copy(k, i, src, dst, peer):
        return section_copy(src, dst, cs.at[k, i], cr.at[k, i], peer)

    to_right, to_left, to_other, far_on, pair_on, far_other = [], [], [], [], [], []
    pair, c_one, c_far, c_two = [], [], [], []
    for k in range(CH):
        to_right.append(b_copy(k, 0, rows(k, OWN), rows(k, LEFT), right))
        to_left.append(b_copy(k, 1, rows(k, OWN), rows(k, RIGHT), left))
        to_other.append(b_copy(k, 2, rows(k, OWN), rows(k, OWN, 1, 1), partner))
        via, onward, near = (LEFT, right, left) if k % 2 == 0 else (RIGHT, left, right)
        far_on.append(b_copy(k, 3, rows(k, via), rows(k, FAR), onward))
        pair_on.append(b_copy(k, 4, rows(k, LEFT, 2), rows(k, LEFT, 2, 1), partner))
        far_other.append(b_copy(k, 5, rows(k, FAR), rows(k, FAR, 1, 1), partner))
        ahead, behind = (RIGHT, LEFT) if k % 2 == 0 else (LEFT, RIGHT)
        pair.append(c_copy(k, 0, p_out.at[k], p_in.at[k], partner))
        c_one.append(c_copy(k, 1, q_out.at[k, pl.ds(R * behind, R)], r_fin.at[k, 0], near))
        c_far.append(c_copy(k, 2, q_out.at[k, pl.ds(R * FAR, R)], r_far.at[k], onward))
        c_two.append(c_copy(k, 3, q_out.at[k, pl.ds(R * ahead, R)], r_fin.at[k, 1], onward))

    def s0(k):
        slabs_in(recv_a, R if k < CH - 1 else R - 1, a_r.at[k])
        from_slabs(recv_a.at[pl.ds(R * k, R)], wide_in.at[k], gat.at[k, pl.ds(0, R)], R)
        first, second = (to_right, to_left) if k % 2 == 0 else (to_left, to_right)
        first[k].start()
        second[k].start()
        to_other[k].start()

    def s1(k):
        first, second = (to_right, to_left) if k % 2 == 0 else (to_left, to_right)
        first[k].wait_recv()
        far_on[k].start()
        second[k].wait_recv()
        pair_on[k].start()

    def s2(k):
        far_on[k].wait_recv()
        far_other[k].start()

    def s3(k):
        to_other[k].wait_recv()
        pair_on[k].wait_recv()
        far_other[k].wait_recv()
        up_out = jnp.dot(gat[k], up_t[...], preferred_element_type=F32)
        hid[k] = jax.nn.gelu(up_out).astype(BF16)
        part = jnp.dot(hid[k], down_v[...], preferred_element_type=F32)
        p_out[k] = part[4 * R :].astype(BF16)
        pair[k].start()
        q_acc[k] = part[: 4 * R]

    def s4(k):
        pair[k].wait_recv()
        ahead, behind = (RIGHT, LEFT) if k % 2 == 0 else (LEFT, RIGHT)

        def summed(g):
            return q_acc[k, pl.ds(R * g, R)] + p_in[k, pl.ds(R * g, R)].astype(F32)

        q_out[k, pl.ds(R * FAR, R)] = summed(FAR).astype(BF16)
        c_far[k].start()
        q_out[k, pl.ds(R * behind, R)] = summed(behind).astype(BF16)
        c_one[k].start()
        for g in (ahead, OWN):
            q_acc[k, pl.ds(R * g, R)] = summed(g)

    def s5(k):
        c_far[k].wait_recv()
        g = RIGHT if k % 2 == 0 else LEFT
        q_out[k, pl.ds(R * g, R)] = (q_acc[k, pl.ds(R * g, R)] + r_far[k].astype(F32)).astype(BF16)
        c_two[k].start()

    def s6(k):
        c_one[k].wait_recv()
        c_two[k].wait_recv()
        result = q_acc[k, pl.ds(0, R)] + r_fin[k, 0].astype(F32) + r_fin[k, 1].astype(F32)
        to_slabs(result, wide_out.at[k], send_d.at[pl.ds(R * k, R)], R)

        def return_row(m, n, base, there):
            e = base + there
            pltpu.make_async_remote_copy(
                send_d.at[m * 4 + n], recv_d.at[me], a2a_s.at[1], d_r.at[0], device_id={"expert": e}, device_id_type=MESH
            ).start()

        def return4(m, c):
            there = (z + 32 - dz_of(m)) % 16
            for n, base in enumerate(by_minus_dy):
                return_row(m, n, base, there)
            return c

        lax.fori_loop(4 * k, min(4 * k + 4, 15), return4, 0)
        if k == CH - 1:
            for n in range(3):
                return_row(15, n, by_minus_dy[n], z)
            recv_d[me] = send_d[E - 1]

    stages = (s0, s1, s2, s3, s4, s5, s6)
    order = "00 10 01 02 20 03 11 30 12 21 40 13 31 22 50 32 41 23 33 42 60 51 43 52 61 53 62 63"
    for step in order.split():
        stages[int(step[0])](int(step[1]))

    for c in to_right + to_left + to_other + far_on + pair_on + far_other + pair + c_one + c_far + c_two:
        c.wait_send()
    slabs_in(send_a, E - 1, a2a_s.at[0])
    slabs_in(send_d, E - 1, a2a_s.at[1])
    slabs_in(recv_d, E - 1, d_r.at[0])
    from_slabs(recv_d, wide, back, E)


def exchange(images, norm_gain, slot_map, logit_scale, up_weight, down_weight):
    any_, vmem = pl.BlockSpec(memory_space=pl.ANY), pl.BlockSpec(memory_space=pltpu.VMEM)
    dma = pltpu.SemaphoreType.DMA
    return pl.pallas_call(
        kernel,
        out_shape=(jax.ShapeDtypeStruct((E, D), BF16), jax.ShapeDtypeStruct((TOK, E), BF16)),
        in_specs=[any_, any_, any_, pl.BlockSpec(memory_space=pltpu.SMEM), any_, any_],
        out_specs=(vmem, vmem),
        scratch_shapes=[
            pltpu.VMEM((TOK, D), BF16), pltpu.VMEM((D,), BF16), pltpu.VMEM((E, D), BF16),
            pltpu.VMEM((FH, D), BF16), pltpu.VMEM((FH, D), BF16), pltpu.VMEM((D, FH), BF16),
            pltpu.VMEM((TOK, D), BF16), pltpu.VMEM((E, 16, 128), F32),
            pltpu.VMEM((CH, R, 16, 128), F32), pltpu.VMEM((CH, R, 16, 128), F32),
            *[pltpu.VMEM((E, SLAB, 128), BF16)] * 4,
            pltpu.VMEM((CH, 8 * R, D), BF16), pltpu.VMEM((CH, 8 * R, FH), BF16), pltpu.VMEM((CH, 4 * R, D), F32),
            pltpu.VMEM((CH, 4 * R, D), BF16), pltpu.VMEM((CH, 4 * R, D), BF16), pltpu.VMEM((CH, 4 * R, D), BF16),
            pltpu.VMEM((CH, R, D), BF16), pltpu.VMEM((CH, 2, R, D), BF16),
            dma((5,)), dma((2,)), dma((CH,)), dma((1,)), dma((CH, 6)), dma((CH, 6)), dma((CH, 4)), dma((CH, 4)),
        ],
        compiler_params=pltpu.CompilerParams(collective_id=0, has_side_effects=True, vmem_limit_bytes=56 * 1024 * 1024),
    )(images, norm_gain, slot_map.T, logit_scale, up_weight, down_weight)


def local(images, norm_gain, slot_map, logit_scale, up_weight, down_weight):
    back, comb = exchange(images, norm_gain, slot_map, logit_scale, up_weight, down_weight)
    mixed = jnp.einsum("te,ed->td", comb, back, preferred_element_type=F32)
    return (images.astype(F32) + mixed[None]).astype(BF16)


def solution(mesh):
    return jax.shard_map(
        local,
        mesh=mesh,
        in_specs=(
            P(("section", "expert"), None, None),
            P(),
            P(),
            P(),
            P("expert", "section", None),
            P("expert", "section", None),
        ),
        out_specs=P(("section", "expert"), None, None),
        check_vma=False,
    )
```

```python
import jax
import jax.numpy as jnp
from jax import lax
from jax.experimental import pallas as pl
from jax.experimental.pallas import tpu as pltpu
from jax.sharding import PartitionSpec as P

epsilon = 1e-06
D = 1408
TOK = 256
E = 64
FH = 640
CH = 4
GROUPS = 4
R = E // CH
GPC = GROUPS // CH
COLS = D // 128
SLAB = 12
F32, BF16 = jnp.float32, jnp.bfloat16
MESH = pl.DeviceIdType.MESH
OWN, LEFT, RIGHT, FAR = 0, 1, 2, 3


def to_slabs(value, wide, slabs, n):
    flat = wide.reshape(n * 16, 128)
    for j in range(COLS):
        flat[pl.ds(j, n, stride=16), :] = value[:, j * 128 : (j + 1) * 128]
    slabs[...] = wide[...][:, :SLAB, :].astype(BF16)


def from_slabs(slabs, wide, out, n):
    wide[:, :SLAB, :] = slabs[...].astype(F32)
    flat = wide.reshape(n * 16, 128)
    for j in range(COLS):
        out[:, j * 128 : (j + 1) * 128] = flat[pl.ds(j, n, stride=16), :].astype(BF16)


def kernel(
    images, gain, slots, scale, up, down,
    back, comb,
    x_v, gain_v, slots_v, up_v, down_v, up_t, normed, wide, wide_in, wide_out,
    send_a, recv_a, send_d, recv_d,
    gat, hid, q_acc, p_out, p_in, q_out, r_fin,
    load_sem, a2a_s, a_r, d_r, bs, br, cs, cr,
):
    sec, me = lax.axis_index("section"), lax.axis_index("expert")
    xs, core = sec // 2, sec % 2
    y, z = me // 16, me % 16
    partner = sec + 1 - 2 * core
    right = ((xs + 1) % 4) * 2 + core
    left = ((xs + 3) % 4) * 2 + core
    far = ((xs + 2) % 4) * 2 + core
    by_dy = [((y + dy) % 4) * 16 for dy in (3, 2, 1, 0)]
    by_minus_dy = [((y + 4 - dy) % 4) * 16 for dy in (3, 2, 1, 0)]

    def dz_of(k, j):
        odd = j % 2
        return (1 - 2 * odd) * (8 - k + (j // 2) * (2 * k - 7)) + odd + 16

    def each_row(k, do):
        def four(j, c):
            for n in range(4):
                do(16 * k + 4 * j + n, n, dz_of(k, j))
            return c

        lax.fori_loop(0, 3 if k == 0 else 4, four, 0)
        if k == 0:
            for n in range(3):
                do(12 + n, n, 16)

    loads = [
        pltpu.make_async_copy(src, dst, load_sem.at[i])
        for i, (src, dst) in enumerate(
            ((slots, slots_v), (gain, gain_v), (images.at[0], x_v), (up.at[0], up_v), (down.at[0], down_v))
        )
    ]
    for c in loads:
        c.start()

    barrier = pltpu.get_barrier_semaphore()

    def greet(e):
        pl.semaphore_signal(barrier, inc=1, device_id={"expert": e}, device_id_type=MESH)

    for g in range(GROUPS):
        each_row(g, lambda i, n, dz: greet(by_dy[n] + (z + dz) % 16))
    for peer in (left, right, far, partner):
        pl.semaphore_signal(barrier, inc=1, device_id={"section": peer}, device_id_type=MESH)

    for c in loads[:3]:
        c.wait()
    x = x_v[...].astype(F32)
    spread = jnp.mean(x * x, axis=-1, keepdims=True)
    normed[...] = (x * lax.rsqrt(spread + epsilon) * gain_v[...].astype(F32).reshape(1, D)).astype(BF16)
    n32 = normed[...].astype(F32)
    token_norm = jnp.sqrt(jnp.sum(n32 * n32, axis=-1, keepdims=True) + epsilon)
    slot_cols = slots_v[...].T
    cols = slot_cols.astype(F32)
    column_norm = jnp.sqrt(jnp.sum(cols * cols, axis=0, keepdims=True) + epsilon)
    raw = jnp.dot(normed[...], slot_cols, preferred_element_type=F32)
    scores = jnp.exp(scale[0] * raw / (token_norm * column_norm))
    dispatch = (scores / jnp.sum(scores, axis=0, keepdims=True)).astype(BF16)
    comb[...] = (scores / jnp.sum(scores, axis=1, keepdims=True)).astype(BF16)
    slot_in = lax.dot_general(dispatch, normed[...], (((0,), (0,)), ((), ())), preferred_element_type=F32)
    to_slabs(slot_in, wide, send_a, E)

    pl.semaphore_wait(barrier, E - 1 + 4)

    def send_row(k, i, e):
        pltpu.make_async_remote_copy(
            send_a.at[e], recv_a.at[i], a2a_s.at[0], a_r.at[k], device_id={"expert": e}, device_id_type=MESH
        ).start()

    for g in range(GROUPS):
        each_row(g, lambda i, n, dz, g=g: send_row(g // GPC, i, by_dy[n] + (z + dz) % 16))
    recv_a[15] = send_a[me]
    for c in loads[3:]:
        c.wait()
    for i in range(FH // 128):
        up_t[:, i * 128 : (i + 1) * 128] = up_v[i * 128 : (i + 1) * 128, :].T

    def slabs_in(buf, n, sem):
        pltpu.make_async_copy(buf.at[pl.ds(0, n)], buf.at[pl.ds(0, n)], sem).wait()

    def section_copy(src, dst, s, r, peer):
        return pltpu.make_async_remote_copy(src, dst, s, r, device_id={"section": peer}, device_id_type=MESH)

    def rows(k, group, n=1, other=0):
        return gat.at[k, pl.ds(4 * R * other + R * group, R * n)]

    def b_copy(k, i, src, dst, peer):
        return section_copy(src, dst, bs.at[k, i], br.at[k, i], peer)

    def c_copy(k, i, group, slot, peer):
        return section_copy(q_out.at[k, pl.ds(R * group, R)], r_fin.at[k, slot], cs.at[k, i], cr.at[k, i], peer)

    hops, to_other, on, pair, sums = ([] for _ in range(5))
    for k in range(CH):
        hops.append([
            b_copy(k, 0, rows(k, OWN), rows(k, FAR), far),
            b_copy(k, 1, rows(k, OWN), rows(k, LEFT), right),
            b_copy(k, 2, rows(k, OWN), rows(k, RIGHT), left),
        ])
        to_other.append(b_copy(k, 3, rows(k, OWN), rows(k, OWN, 1, 1), partner))
        on.append(b_copy(k, 4, rows(k, LEFT, 3), rows(k, LEFT, 3, 1), partner))
        pair.append(section_copy(p_out.at[k], p_in.at[k], cs.at[k, 0], cr.at[k, 0], partner))
        sums.append([c_copy(k, 1, FAR, 2, far), c_copy(k, 2, LEFT, 0, left), c_copy(k, 3, RIGHT, 1, right)])

    def s0(k):
        slabs_in(recv_a, R if k else R - 1, a_r.at[k])
        from_slabs(recv_a.at[pl.ds(R * k, R)], wide_in.at[k], gat.at[k, pl.ds(0, R)], R)
        for c in hops[k]:
            c.start()
        to_other[k].start()

    def s1(k):
        for c in hops[k]:
            c.wait_recv()
        on[k].start()

    def s2(k):
        to_other[k].wait_recv()
        on[k].wait_recv()
        up_out = jnp.dot(gat[k], up_t[...], preferred_element_type=F32)
        hid[k] = jax.nn.gelu(up_out).astype(BF16)
        part = jnp.dot(hid[k], down_v[...], preferred_element_type=F32)
        p_out[k] = part[4 * R :].astype(BF16)
        pair[k].start()
        q_acc[k] = part[: 4 * R]

    def s3(k):
        pair[k].wait_recv()
        for group, c in zip((FAR, LEFT, RIGHT), sums[k]):
            at = pl.ds(R * group, R)
            q_out[k, at] = (q_acc[k, at] + p_in[k, at].astype(F32)).astype(BF16)
            c.start()
        q_acc[k, pl.ds(0, R)] = q_acc[k, pl.ds(0, R)] + p_in[k, pl.ds(0, R)].astype(F32)

    def s4(k):
        for c in sums[k]:
            c.wait_recv()
        r0, r1, r2 = (r_fin[k, n].astype(F32) for n in range(3))
        result = (q_acc[k, pl.ds(0, R)] + r0) + (r1 + r2)
        to_slabs(result, wide_out.at[k], send_d.at[pl.ds(R * k, R)], R)

        def return_row(i, e):
            pltpu.make_async_remote_copy(
                send_d.at[i], recv_d.at[me], a2a_s.at[1], d_r.at[0], device_id={"expert": e}, device_id_type=MESH
            ).start()

        for g in range(GPC * k, GPC * (k + 1)):
            each_row(g, lambda i, n, dz: return_row(i, by_minus_dy[n] + (z + 32 - dz) % 16))
        if k == 0:
            recv_d[me] = send_d[15]

    stages = (s0, s1, s2, s3, s4)
    order = (0, 1, 10, 2, 20, 11, 3, 30, 21, 12, 31, 22, 13, 40, 32, 23, 41, 33, 42, 43)
    for step in order:
        stages[step // 10](step % 10)

    for c in to_other + on + pair + sum(hops + sums, []):
        c.wait_send()
    slabs_in(send_a, E - 1, a2a_s.at[0])
    slabs_in(send_d, E - 1, a2a_s.at[1])
    slabs_in(recv_d, E - 1, d_r.at[0])
    from_slabs(recv_d, wide, back, E)


def exchange(images, norm_gain, slot_map, logit_scale, up_weight, down_weight):
    hbm, vmem = pl.BlockSpec(memory_space=pl.ANY), pl.BlockSpec(memory_space=pltpu.VMEM)
    dma = pltpu.SemaphoreType.DMA
    return pl.pallas_call(
        kernel,
        out_shape=(jax.ShapeDtypeStruct((E, D), BF16), jax.ShapeDtypeStruct((TOK, E), BF16)),
        in_specs=[hbm, hbm, hbm, pl.BlockSpec(memory_space=pltpu.SMEM), hbm, hbm],
        out_specs=(vmem, vmem),
        scratch_shapes=[
            pltpu.VMEM((TOK, D), BF16), pltpu.VMEM((D,), BF16), pltpu.VMEM((E, D), BF16),
            pltpu.VMEM((FH, D), BF16), pltpu.VMEM((FH, D), BF16), pltpu.VMEM((D, FH), BF16),
            pltpu.VMEM((TOK, D), BF16), pltpu.VMEM((E, 16, 128), F32),
            pltpu.VMEM((CH, R, 16, 128), F32), pltpu.VMEM((CH, R, 16, 128), F32),
            *[pltpu.VMEM((E, SLAB, 128), BF16)] * 4,
            pltpu.VMEM((CH, 8 * R, D), BF16), pltpu.VMEM((CH, 8 * R, FH), BF16), pltpu.VMEM((CH, 4 * R, D), F32),
            pltpu.VMEM((CH, 4 * R, D), BF16), pltpu.VMEM((CH, 4 * R, D), BF16), pltpu.VMEM((CH, 4 * R, D), BF16),
            pltpu.VMEM((CH, 3, R, D), BF16),
            dma((5,)), dma((2,)), dma((CH,)), dma((1,)), dma((CH, 5)), dma((CH, 5)), dma((CH, 4)), dma((CH, 4)),
        ],
        compiler_params=pltpu.CompilerParams(collective_id=0, has_side_effects=True, vmem_limit_bytes=56 * 1024 * 1024),
    )(images, norm_gain, slot_map.T, logit_scale, up_weight, down_weight)


def local(images, norm_gain, slot_map, logit_scale, up_weight, down_weight):
    back, comb = exchange(images, norm_gain, slot_map, logit_scale, up_weight, down_weight)
    mixed = jnp.einsum("te,ed->td", comb, back, preferred_element_type=F32)
    return (images.astype(F32) + mixed[None]).astype(BF16)


def solution(mesh):
    return jax.shard_map(
        local,
        mesh=mesh,
        in_specs=(
            P(("section", "expert"), None, None),
            P(),
            P(),
            P(),
            P("expert", "section", None),
            P("expert", "section", None),
        ),
        out_specs=P(("section", "expert"), None, None),
        check_vma=False,
    )
```

```python
import jax
import jax.numpy as jnp
from jax import lax
from jax.experimental import pallas as pl
from jax.experimental.pallas import tpu as pltpu
from jax.sharding import PartitionSpec as P

epsilon = 1e-06
D = 1408
TOK = 256
E = 64
FH = 640
CH = 4
GROUPS = 4
R = E // CH
GPC = GROUPS // CH
ORDER = (0, 1, 2, 3)
COLS = D // 128
SLAB = 12
F32, BF16 = jnp.float32, jnp.bfloat16
MESH = pl.DeviceIdType.MESH
OWN, LEFT, RIGHT, FAR = 0, 1, 2, 3


def to_slabs(value, wide, slabs, n):
    flat = wide.reshape(n * 16, 128)
    for j in range(COLS):
        flat[pl.ds(j, n, stride=16), :] = value[:, j * 128 : (j + 1) * 128]
    slabs[...] = wide[...][:, :SLAB, :].astype(BF16)


def from_slabs(slabs, wide, out, n):
    wide[:, :SLAB, :] = slabs[...].astype(F32)
    flat = wide.reshape(n * 16, 128)
    for j in range(COLS):
        out[:, j * 128 : (j + 1) * 128] = flat[pl.ds(j, n, stride=16), :].astype(BF16)


def kernel(
    images, gain, slots, scale, up, down,
    back, comb,
    x_v, gain_v, slots_v, up_v, down_v, up_t, normed, wide, wide_in, wide_out,
    send_a, recv_a, send_d, recv_d,
    gat, hid, q_acc, p_out, p_in, q_out, r_fin,
    load_sem, a2a_s, a_r, d_r, bs, br, cs, cr,
):
    sec, me = lax.axis_index("section"), lax.axis_index("expert")
    xs, core = sec // 2, sec % 2
    y, z = me // 16, me % 16
    partner = sec + 1 - 2 * core
    right = ((xs + 1) % 4) * 2 + core
    left = ((xs + 3) % 4) * 2 + core
    far = ((xs + 2) % 4) * 2 + core
    def each_row(k, do):
        g = ORDER[k]

        def body(n, c):
            for j, dz in enumerate((8 - g, g - 7, g + 1, -g)):
                do(16 * k + 4 * j + n, 3 - n, dz)
            return c

        lax.fori_loop(0, 4, body, 0)

    def other_core(e):
        return {"section": partner, "expert": e}

    def at_offset(dy, dz):
        return ((y + dy + 4) % 4) * 16 + (z + dz + 16) % 16

    loads = [
        pltpu.make_async_copy(src, dst, load_sem.at[i])
        for i, (src, dst) in enumerate(
            ((slots, slots_v), (gain, gain_v), (images.at[0], x_v), (up.at[0], up_v), (down.at[0], down_v))
        )
    ]
    for c in loads:
        c.start()

    barrier = pltpu.get_barrier_semaphore()

    def greet(e):
        pl.semaphore_signal(barrier, inc=1, device_id=other_core(e), device_id_type=MESH)

    for g in range(GROUPS):
        each_row(g, lambda i, dy, dz: greet(at_offset(dy, dz)))
    for peer in (left, right, far):
        pl.semaphore_signal(barrier, inc=1, device_id={"section": peer}, device_id_type=MESH)

    for c in loads[:3]:
        c.wait()
    x = x_v[...].astype(F32)
    spread = jnp.mean(x * x, axis=-1, keepdims=True)
    normed[...] = (x * lax.rsqrt(spread + epsilon) * gain_v[...].astype(F32).reshape(1, D)).astype(BF16)
    n32 = normed[...].astype(F32)
    token_norm = jnp.sqrt(jnp.sum(n32 * n32, axis=-1, keepdims=True) + epsilon)
    slot_cols = slots_v[...].T
    cols = slot_cols.astype(F32)
    column_norm = jnp.sqrt(jnp.sum(cols * cols, axis=0, keepdims=True) + epsilon)
    raw = jnp.dot(normed[...], slot_cols, preferred_element_type=F32)
    scores = jnp.exp(scale[0] * raw / (token_norm * column_norm))
    dispatch = (scores / jnp.sum(scores, axis=0, keepdims=True)).astype(BF16)
    comb[...] = (scores / jnp.sum(scores, axis=1, keepdims=True)).astype(BF16)
    slot_in = lax.dot_general(dispatch, normed[...], (((0,), (0,)), ((), ())), preferred_element_type=F32)
    to_slabs(slot_in, wide, send_a, E)

    pl.semaphore_wait(barrier, E + 3)

    def send_row(k, i, e):
        pltpu.make_async_remote_copy(
            send_a.at[e], recv_a.at[i], a2a_s.at[0], a_r.at[k], device_id=other_core(e), device_id_type=MESH
        ).start()

    for g in range(GROUPS):
        each_row(g, lambda i, dy, dz, g=g: send_row(g // GPC, i, at_offset(dy, dz)))
    for c in loads[3:]:
        c.wait()
    for i in range(FH // 128):
        up_t[:, i * 128 : (i + 1) * 128] = up_v[i * 128 : (i + 1) * 128, :].T

    def slabs_in(buf, n, sem):
        pltpu.make_async_copy(buf.at[pl.ds(0, n)], buf.at[pl.ds(0, n)], sem).wait()

    def section_copy(src, dst, s, r, peer):
        return pltpu.make_async_remote_copy(src, dst, s, r, device_id={"section": peer}, device_id_type=MESH)

    def rows(k, group, n=1, other=0):
        return gat.at[k, pl.ds(4 * R * other + R * group, R * n)]

    def b_copy(k, i, src, dst, peer):
        return section_copy(src, dst, bs.at[k, i], br.at[k, i], peer)

    def c_copy(k, i, group, slot, peer):
        return section_copy(q_out.at[k, pl.ds(R * group, R)], r_fin.at[k, slot], cs.at[k, i], cr.at[k, i], peer)

    hops, to_other, on, pair, sums = ([] for _ in range(5))
    for k in range(CH):
        hops.append([
            b_copy(k, 0, rows(k, OWN), rows(k, FAR), far),
            b_copy(k, 1, rows(k, OWN), rows(k, LEFT), right),
            b_copy(k, 2, rows(k, OWN), rows(k, RIGHT), left),
        ])
        to_other.append(b_copy(k, 3, rows(k, OWN), rows(k, OWN, 1, 1), partner))
        on.append(b_copy(k, 4, rows(k, LEFT, 3), rows(k, LEFT, 3, 1), partner))
        pair.append(section_copy(p_out.at[k], p_in.at[k], cs.at[k, 0], cr.at[k, 0], partner))
        sums.append([c_copy(k, 1, FAR, 2, far), c_copy(k, 2, LEFT, 0, left), c_copy(k, 3, RIGHT, 1, right)])

    def s0(k):
        slabs_in(recv_a, R, a_r.at[k])
        from_slabs(recv_a.at[pl.ds(R * k, R)], wide_in.at[k], gat.at[k, pl.ds(0, R)], R)
        for c in hops[k]:
            c.start()
        to_other[k].start()

    def s1(k):
        for c in hops[k]:
            c.wait_recv()
        on[k].start()

    def s2(k):
        to_other[k].wait_recv()
        on[k].wait_recv()
        up_out = jnp.dot(gat[k], up_t[...], preferred_element_type=F32)
        hid[k] = jax.nn.gelu(up_out).astype(BF16)
        part = jnp.dot(hid[k], down_v[...], preferred_element_type=F32)
        p_out[k] = part[4 * R :].astype(BF16)
        pair[k].start()
        q_acc[k] = part[: 4 * R]

    def s3(k):
        pair[k].wait_recv()
        for group, c in zip((FAR, LEFT, RIGHT), sums[k]):
            at = pl.ds(R * group, R)
            q_out[k, at] = (q_acc[k, at] + p_in[k, at].astype(F32)).astype(BF16)
            c.start()
        q_acc[k, pl.ds(0, R)] = q_acc[k, pl.ds(0, R)] + p_in[k, pl.ds(0, R)].astype(F32)

    def s4(k):
        for c in sums[k]:
            c.wait_recv()
        r0, r1, r2 = (r_fin[k, n].astype(F32) for n in range(3))
        result = (q_acc[k, pl.ds(0, R)] + r0) + (r1 + r2)
        to_slabs(result, wide_out.at[k], send_d.at[pl.ds(R * k, R)], R)

        def return_row(i, e):
            pltpu.make_async_remote_copy(
                send_d.at[i], recv_d.at[me], a2a_s.at[1], d_r.at[0], device_id=other_core(e), device_id_type=MESH
            ).start()

        for g in range(GPC * k, GPC * (k + 1)):
            each_row(g, lambda i, dy, dz: return_row(i, at_offset(-dy, -dz)))

    stages = (s0, s1, s2, s3, s4)
    order = (0, 1, 10, 2, 20, 11, 3, 30, 21, 12, 31, 22, 13, 32, 23, 40, 33, 41, 42, 43)
    for step in order:
        stages[step // 10](step % 10)

    for c in to_other + on + pair + sum(hops + sums, []):
        c.wait_send()
    slabs_in(send_a, E, a2a_s.at[0])
    slabs_in(send_d, E, a2a_s.at[1])
    slabs_in(recv_d, E, d_r.at[0])
    from_slabs(recv_d, wide, back, E)


def in_hbm(array):
    return pltpu.with_memory_space_constraint(array, pltpu.HBM)


def exchange(images, norm_gain, slot_map, logit_scale, up_weight, down_weight):
    hbm, vmem = pl.BlockSpec(memory_space=pl.ANY), pl.BlockSpec(memory_space=pltpu.VMEM)
    dma = pltpu.SemaphoreType.DMA
    return pl.pallas_call(
        kernel,
        out_shape=(jax.ShapeDtypeStruct((E, D), BF16), jax.ShapeDtypeStruct((TOK, E), BF16)),
        in_specs=[hbm, hbm, hbm, pl.BlockSpec(memory_space=pltpu.SMEM), hbm, hbm],
        out_specs=(vmem, vmem),
        scratch_shapes=[
            pltpu.VMEM((TOK, D), BF16), pltpu.VMEM((D,), BF16), pltpu.VMEM((E, D), BF16),
            pltpu.VMEM((FH, D), BF16), pltpu.VMEM((FH, D), BF16), pltpu.VMEM((D, FH), BF16),
            pltpu.VMEM((TOK, D), BF16), pltpu.VMEM((E, 16, 128), F32),
            pltpu.VMEM((CH, R, 16, 128), F32), pltpu.VMEM((CH, R, 16, 128), F32),
            *[pltpu.VMEM((E, SLAB, 128), BF16)] * 4,
            pltpu.VMEM((CH, 8 * R, D), BF16), pltpu.VMEM((CH, 8 * R, FH), BF16), pltpu.VMEM((CH, 4 * R, D), F32),
            pltpu.VMEM((CH, 4 * R, D), BF16), pltpu.VMEM((CH, 4 * R, D), BF16), pltpu.VMEM((CH, 4 * R, D), BF16),
            pltpu.VMEM((CH, 3, R, D), BF16),
            dma((5,)), dma((2,)), dma((CH,)), dma((1,)), dma((CH, 5)), dma((CH, 5)), dma((CH, 4)), dma((CH, 4)),
        ],
        compiler_params=pltpu.CompilerParams(collective_id=0, has_side_effects=True, vmem_limit_bytes=52 * 1024 * 1024),
    )(in_hbm(images), in_hbm(norm_gain), in_hbm(slot_map.T), logit_scale, in_hbm(up_weight), in_hbm(down_weight))


def local(images, norm_gain, slot_map, logit_scale, up_weight, down_weight):
    back, comb = exchange(images, norm_gain, slot_map, logit_scale, up_weight, down_weight)
    mixed = jnp.einsum("te,ed->td", comb, back, preferred_element_type=F32)
    return (images.astype(F32) + mixed[None]).astype(BF16)


def solution(mesh):
    return jax.shard_map(
        local,
        mesh=mesh,
        in_specs=(
            P(("section", "expert"), None, None),
            P(),
            P(),
            P(),
            P("expert", "section", None),
            P("expert", "section", None),
        ),
        out_specs=P(("section", "expert"), None, None),
        check_vma=False,
    )
```

```python
import jax
import jax.numpy as jnp
from jax import lax
from jax.experimental import pallas as pl
from jax.experimental.pallas import tpu as pltpu
from jax.sharding import PartitionSpec as P

epsilon = 1e-06
D = 1408
TOK = 256
E = 64
FH = 640
CH = 4
GROUPS = 4
R = E // CH
GPC = GROUPS // CH
ORDER = (0, 1, 2, 3)
COLS = D // 128
SLAB = 11
F32, BF16 = jnp.float32, jnp.bfloat16
MESH = pl.DeviceIdType.MESH
OWN, LEFT, RIGHT, FAR = 0, 1, 2, 3


def to_slabs(value, wide, slabs, n):
    flat = wide.reshape(n * 16, 128)
    for j in range(COLS):
        flat[pl.ds(j, n, stride=16), :] = value[:, j * 128 : (j + 1) * 128]
    slabs[...] = wide[...][:, :SLAB, :].astype(BF16)


def from_slabs(slabs, wide, out, n):
    wide[:, :SLAB, :] = slabs[...].astype(F32)
    flat = wide.reshape(n * 16, 128)
    for j in range(COLS):
        out[:, j * 128 : (j + 1) * 128] = flat[pl.ds(j, n, stride=16), :].astype(BF16)


def kernel(
    images, gain, slots, scale, up, down,
    back, comb,
    x_v, gain_v, slots_v, up_v, down_v, up_t, normed, wide, wide_in, wide_out,
    send_a, recv_a, send_d, recv_d,
    gat, hid, q_acc, p_out, p_in, q_out, r_fin,
    load_sem, a2a_s, a_r, d_r, bs, br, cs, cr,
):
    sec, me = lax.axis_index("section"), lax.axis_index("expert")
    xs, core = sec // 2, sec % 2
    y, z = me // 16, me % 16
    partner = sec + 1 - 2 * core
    right = ((xs + 1) % 4) * 2 + core
    left = ((xs + 3) % 4) * 2 + core
    far = ((xs + 2) % 4) * 2 + core
    def each_row(k, do):
        g = ORDER[k]

        def body(n, c):
            for j, dz in enumerate((8 - g, g - 7, g + 1, -g)):
                do(16 * k + 4 * j + n, 3 - n, dz)
            return c

        lax.fori_loop(0, 4, body, 0)

    def other_core(e):
        return {"section": partner, "expert": e}

    def at_offset(dy, dz):
        return ((y + dy + 4) % 4) * 16 + (z + dz + 16) % 16

    loads = [
        pltpu.make_async_copy(src, dst, load_sem.at[i])
        for i, (src, dst) in enumerate(
            ((slots, slots_v), (gain, gain_v), (images.at[0], x_v), (up.at[0], up_v), (down.at[0], down_v))
        )
    ]
    for c in loads:
        c.start()

    barrier = pltpu.get_barrier_semaphore()

    def greet(e):
        pl.semaphore_signal(barrier, inc=1, device_id=other_core(e), device_id_type=MESH)

    for g in range(GROUPS):
        each_row(g, lambda i, dy, dz: greet(at_offset(dy, dz)))
    for peer in (left, right, far):
        pl.semaphore_signal(barrier, inc=1, device_id={"section": peer}, device_id_type=MESH)

    for c in loads[:3]:
        c.wait()
    x = x_v[...].astype(F32)
    spread = jnp.mean(x * x, axis=-1, keepdims=True)
    normed[...] = (x * lax.rsqrt(spread + epsilon) * gain_v[...].astype(F32).reshape(1, D)).astype(BF16)
    n32 = normed[...].astype(F32)
    token_norm = jnp.sqrt(jnp.sum(n32 * n32, axis=-1, keepdims=True) + epsilon)
    slot_cols = slots_v[...].T
    cols = slot_cols.astype(F32)
    column_norm = jnp.sqrt(jnp.sum(cols * cols, axis=0, keepdims=True) + epsilon)
    raw = jnp.dot(normed[...], slot_cols, preferred_element_type=F32)
    scores = jnp.exp(scale[0] * raw / (token_norm * column_norm))
    dispatch = (scores / jnp.sum(scores, axis=0, keepdims=True)).astype(BF16)
    comb[...] = (scores / jnp.sum(scores, axis=1, keepdims=True)).astype(BF16)
    slot_in = lax.dot_general(dispatch, normed[...], (((0,), (0,)), ((), ())), preferred_element_type=F32)
    to_slabs(slot_in, wide, send_a, E)

    pl.semaphore_wait(barrier, E + 3)

    def send_row(k, i, e):
        pltpu.make_async_remote_copy(
            send_a.at[e], recv_a.at[i], a2a_s.at[0], a_r.at[k], device_id=other_core(e), device_id_type=MESH
        ).start()

    for g in range(GROUPS):
        each_row(g, lambda i, dy, dz, g=g: send_row(g // GPC, i, at_offset(dy, dz)))
    for c in loads[3:]:
        c.wait()
    for i in range(FH // 128):
        up_t[:, i * 128 : (i + 1) * 128] = up_v[i * 128 : (i + 1) * 128, :].T

    def slabs_in(buf, n, sem):
        pltpu.make_async_copy(buf.at[pl.ds(0, n)], buf.at[pl.ds(0, n)], sem).wait()

    def section_copy(src, dst, s, r, peer):
        return pltpu.make_async_remote_copy(src, dst, s, r, device_id={"section": peer}, device_id_type=MESH)

    def rows(k, group, n=1, other=0):
        return gat.at[k, pl.ds(4 * R * other + R * group, R * n)]

    def b_copy(k, i, src, dst, peer):
        return section_copy(src, dst, bs.at[k, i], br.at[k, i], peer)

    def c_copy(k, i, group, slot, peer):
        return section_copy(q_out.at[k, pl.ds(R * group, R)], r_fin.at[k, slot], cs.at[k, i], cr.at[k, i], peer)

    hops, to_other, on, pair, sums = ([] for _ in range(5))
    for k in range(CH):
        hops.append([
            b_copy(k, 0, rows(k, OWN), rows(k, FAR), far),
            b_copy(k, 1, rows(k, OWN), rows(k, LEFT), right),
            b_copy(k, 2, rows(k, OWN), rows(k, RIGHT), left),
        ])
        to_other.append(b_copy(k, 3, rows(k, OWN), rows(k, OWN, 1, 1), partner))
        on.append([
            b_copy(k, 4, rows(k, LEFT, 2), rows(k, LEFT, 2, 1), partner),
            b_copy(k, 5, rows(k, FAR), rows(k, FAR, 1, 1), partner),
        ])
        pair.append(section_copy(p_out.at[k], p_in.at[k], cs.at[k, 0], cr.at[k, 0], partner))
        sums.append([c_copy(k, 1, FAR, 2, far), c_copy(k, 2, LEFT, 0, left), c_copy(k, 3, RIGHT, 1, right)])

    def s0(k):
        slabs_in(recv_a, R, a_r.at[k])
        from_slabs(recv_a.at[pl.ds(R * k, R)], wide_in.at[k], gat.at[k, pl.ds(0, R)], R)
        for c in hops[k]:
            c.start()
        to_other[k].start()

    def s1(k):
        hops[k][1].wait_recv()
        hops[k][2].wait_recv()
        on[k][0].start()
        hops[k][0].wait_recv()
        on[k][1].start()

    def s2(k):
        to_other[k].wait_recv()
        for c in on[k]:
            c.wait_recv()
        up_out = jnp.dot(gat[k], up_t[...], preferred_element_type=F32)
        hid[k] = jax.nn.gelu(up_out).astype(BF16)
        part = jnp.dot(hid[k], down_v[...], preferred_element_type=F32)
        p_out[k] = part[4 * R :].astype(BF16)
        pair[k].start()
        q_acc[k] = part[: 4 * R]

    def s3(k):
        pair[k].wait_recv()
        for group, c in zip((FAR, LEFT, RIGHT), sums[k]):
            at = pl.ds(R * group, R)
            q_out[k, at] = (q_acc[k, at] + p_in[k, at].astype(F32)).astype(BF16)
            c.start()
        q_acc[k, pl.ds(0, R)] = q_acc[k, pl.ds(0, R)] + p_in[k, pl.ds(0, R)].astype(F32)

    def s4(k):
        for c in sums[k]:
            c.wait_recv()
        r0, r1, r2 = (r_fin[k, n].astype(F32) for n in range(3))
        result = (q_acc[k, pl.ds(0, R)] + r0) + (r1 + r2)
        to_slabs(result, wide_out.at[k], send_d.at[pl.ds(R * k, R)], R)

        def return_row(i, e):
            pltpu.make_async_remote_copy(
                send_d.at[i], recv_d.at[me], a2a_s.at[1], d_r.at[0], device_id=other_core(e), device_id_type=MESH
            ).start()

        for g in range(GPC * k, GPC * (k + 1)):
            each_row(g, lambda i, dy, dz: return_row(i, at_offset(-dy, -dz)))

    stages = (s0, s1, s2, s3, s4)
    order = (0, 1, 10, 2, 20, 11, 30, 3, 21, 31, 12, 22, 40, 13, 32, 23, 41, 33, 42, 43)
    for step in order:
        stages[step // 10](step % 10)

    for c in to_other + pair + sum(hops + on + sums, []):
        c.wait_send()
    slabs_in(send_a, E, a2a_s.at[0])
    slabs_in(send_d, E, a2a_s.at[1])
    slabs_in(recv_d, E, d_r.at[0])
    from_slabs(recv_d, wide, back, E)


def in_hbm(array):
    return pltpu.with_memory_space_constraint(array, pltpu.HBM)


def exchange(images, norm_gain, slot_map, logit_scale, up_weight, down_weight):
    hbm, vmem = pl.BlockSpec(memory_space=pl.ANY), pl.BlockSpec(memory_space=pltpu.VMEM)
    dma = pltpu.SemaphoreType.DMA
    return pl.pallas_call(
        kernel,
        out_shape=(jax.ShapeDtypeStruct((E, D), BF16), jax.ShapeDtypeStruct((TOK, E), BF16)),
        in_specs=[hbm, hbm, hbm, pl.BlockSpec(memory_space=pltpu.SMEM), hbm, hbm],
        out_specs=(vmem, vmem),
        scratch_shapes=[
            pltpu.VMEM((TOK, D), BF16), pltpu.VMEM((D,), BF16), pltpu.VMEM((E, D), BF16),
            pltpu.VMEM((FH, D), BF16), pltpu.VMEM((FH, D), BF16), pltpu.VMEM((D, FH), BF16),
            pltpu.VMEM((TOK, D), BF16), pltpu.VMEM((E, 16, 128), F32),
            pltpu.VMEM((CH, R, 16, 128), F32), pltpu.VMEM((CH, R, 16, 128), F32),
            *[pltpu.VMEM((E, SLAB, 128), BF16)] * 4,
            pltpu.VMEM((CH, 8 * R, D), BF16), pltpu.VMEM((CH, 8 * R, FH), BF16), pltpu.VMEM((CH, 4 * R, D), F32),
            pltpu.VMEM((CH, 4 * R, D), BF16), pltpu.VMEM((CH, 4 * R, D), BF16), pltpu.VMEM((CH, 4 * R, D), BF16),
            pltpu.VMEM((CH, 3, R, D), BF16),
            dma((5,)), dma((2,)), dma((CH,)), dma((1,)), dma((CH, 6)), dma((CH, 6)), dma((CH, 4)), dma((CH, 4)),
        ],
        compiler_params=pltpu.CompilerParams(collective_id=0, has_side_effects=True, vmem_limit_bytes=52 * 1024 * 1024),
    )(in_hbm(images), in_hbm(norm_gain), in_hbm(slot_map.T), logit_scale, in_hbm(up_weight), in_hbm(down_weight))


def local(images, norm_gain, slot_map, logit_scale, up_weight, down_weight):
    back, comb = exchange(images, norm_gain, slot_map, logit_scale, up_weight, down_weight)
    mixed = jnp.einsum("te,ed->td", comb, back, preferred_element_type=F32)
    return (images.astype(F32) + mixed[None]).astype(BF16)


def solution(mesh):
    return jax.shard_map(
        local,
        mesh=mesh,
        in_specs=(
            P(("section", "expert"), None, None),
            P(),
            P(),
            P(),
            P("expert", "section", None),
            P("expert", "section", None),
        ),
        out_specs=P(("section", "expert"), None, None),
        check_vma=False,
    )
```

```python
import jax
import jax.numpy as jnp
from jax import lax
from jax.experimental import pallas as pl
from jax.experimental.pallas import tpu as pltpu
from jax.sharding import PartitionSpec as P

epsilon = 1e-06
D = 1408
TOK = 256
E = 64
FH = 640
CH = 4
GROUPS = 4
R = E // CH
GPC = GROUPS // CH
ORDER = (0, 1, 2, 3)
COLS = D // 128
SLAB = 11
F32, BF16 = jnp.float32, jnp.bfloat16
MESH = pl.DeviceIdType.MESH
OWN, LEFT, RIGHT, FAR = 0, 1, 2, 3


def to_slabs(value, wide, slabs, n):
    flat = wide.reshape(n * 16, 128)
    for j in range(COLS):
        flat[pl.ds(j, n, stride=16), :] = value[:, j * 128 : (j + 1) * 128]
    slabs[...] = wide[...][:, :SLAB, :].astype(BF16)


def from_slabs(slabs, wide, out, n):
    wide[:, :SLAB, :] = slabs[...].astype(F32)
    flat = wide.reshape(n * 16, 128)
    for j in range(COLS):
        out[:, j * 128 : (j + 1) * 128] = flat[pl.ds(j, n, stride=16), :].astype(BF16)


def kernel(
    images, gain, slots, scale, up, down,
    back, comb,
    x_v, gain_v, slots_v, up_v, down_v, up_t, normed, wide, wide_in, wide_out,
    send_a, recv_a, send_d, recv_d,
    gat, hid, q_acc, p_out, p_in, q_out, r_fin,
    load_sem, a2a_s, a_r, d_r, bs, br, cs, cr,
):
    sec, me = lax.axis_index("section"), lax.axis_index("expert")
    xs, core = sec // 2, sec % 2
    y, z = me // 16, me % 16
    partner = sec + 1 - 2 * core
    right = ((xs + 1) % 4) * 2 + 1 - core
    left = ((xs + 3) % 4) * 2 + 1 - core
    far = ((xs + 2) % 4) * 2 + 1 - core
    def each_row(k, do):
        g = ORDER[k]

        def body(n, c):
            for j, dz in enumerate((8 - g, g - 7, g + 1, -g)):
                do(16 * k + 4 * j + n, 3 - n, dz)
            return c

        lax.fori_loop(0, 4, body, 0)

    def other_core(e):
        return {"section": partner, "expert": e}

    def at_offset(dy, dz):
        return ((y + dy + 4) % 4) * 16 + (z + dz + 16) % 16

    loads = [
        pltpu.make_async_copy(src, dst, load_sem.at[i])
        for i, (src, dst) in enumerate(
            ((slots, slots_v), (gain, gain_v), (images.at[0], x_v), (up.at[0], up_v), (down.at[0], down_v))
        )
    ]
    for c in loads:
        c.start()

    barrier = pltpu.get_barrier_semaphore()

    def greet(e):
        pl.semaphore_signal(barrier, inc=1, device_id=other_core(e), device_id_type=MESH)

    for g in range(GROUPS):
        each_row(g, lambda i, dy, dz: greet(at_offset(dy, dz)))
    for peer in (left, right, far):
        pl.semaphore_signal(barrier, inc=1, device_id={"section": peer}, device_id_type=MESH)

    for c in loads[:3]:
        c.wait()
    x = x_v[...].astype(F32)
    spread = jnp.mean(x * x, axis=-1, keepdims=True)
    normed[...] = (x * lax.rsqrt(spread + epsilon) * gain_v[...].astype(F32).reshape(1, D)).astype(BF16)
    n32 = normed[...].astype(F32)
    token_norm = jnp.sqrt(jnp.sum(n32 * n32, axis=-1, keepdims=True) + epsilon)
    slot_cols = slots_v[...].T
    cols = slot_cols.astype(F32)
    column_norm = jnp.sqrt(jnp.sum(cols * cols, axis=0, keepdims=True) + epsilon)
    raw = jnp.dot(normed[...], slot_cols, preferred_element_type=F32)
    scores = jnp.exp(scale[0] * raw / (token_norm * column_norm))
    dispatch = (scores / jnp.sum(scores, axis=0, keepdims=True)).astype(BF16)
    comb[...] = (scores / jnp.sum(scores, axis=1, keepdims=True)).astype(BF16)
    slot_in = lax.dot_general(dispatch, normed[...], (((0,), (0,)), ((), ())), preferred_element_type=F32)
    to_slabs(slot_in, wide, send_a, E)

    pl.semaphore_wait(barrier, E + 3)

    def send_row(k, i, e):
        pltpu.make_async_remote_copy(
            send_a.at[e], recv_a.at[i], a2a_s.at[0], a_r.at[k], device_id=other_core(e), device_id_type=MESH
        ).start()

    for g in range(GROUPS):
        each_row(g, lambda i, dy, dz, g=g: send_row(g // GPC, i, at_offset(dy, dz)))
    for c in loads[3:]:
        c.wait()
    for i in range(FH // 128):
        up_t[:, i * 128 : (i + 1) * 128] = up_v[i * 128 : (i + 1) * 128, :].T

    def slabs_in(buf, n, sem):
        pltpu.make_async_copy(buf.at[pl.ds(0, n)], buf.at[pl.ds(0, n)], sem).wait()

    def section_copy(src, dst, s, r, peer):
        return pltpu.make_async_remote_copy(src, dst, s, r, device_id={"section": peer}, device_id_type=MESH)

    def rows(k, group, n=1, other=0):
        return gat.at[k, pl.ds(4 * R * other + R * group, R * n)]

    def b_copy(k, i, src, dst, peer):
        return section_copy(src, dst, bs.at[k, i], br.at[k, i], peer)

    def c_copy(k, i, group, slot, peer):
        return section_copy(q_out.at[k, pl.ds(R * group, R)], r_fin.at[k, slot], cs.at[k, i], cr.at[k, i], peer)

    hops, to_other, on, pair, sums = ([] for _ in range(5))
    for k in range(CH):
        hops.append([
            b_copy(k, 0, rows(k, OWN), rows(k, FAR), far),
            b_copy(k, 1, rows(k, OWN), rows(k, LEFT), right),
            b_copy(k, 2, rows(k, OWN), rows(k, RIGHT), left),
        ])
        to_other.append(b_copy(k, 3, rows(k, OWN), rows(k, OWN, 1, 1), partner))
        on.append([
            b_copy(k, 4, rows(k, LEFT, 2), rows(k, LEFT, 2, 1), partner),
            b_copy(k, 5, rows(k, FAR), rows(k, FAR, 1, 1), partner),
        ])
        pair.append(section_copy(p_out.at[k], p_in.at[k], cs.at[k, 0], cr.at[k, 0], partner))
        sums.append([c_copy(k, 1, FAR, 2, far), c_copy(k, 2, LEFT, 0, left), c_copy(k, 3, RIGHT, 1, right)])

    def s0(k):
        slabs_in(recv_a, R, a_r.at[k])
        from_slabs(recv_a.at[pl.ds(R * k, R)], wide_in.at[k], gat.at[k, pl.ds(0, R)], R)
        for c in hops[k]:
            c.start()
        to_other[k].start()

    def s1(k):
        hops[k][1].wait_recv()
        hops[k][2].wait_recv()
        on[k][0].start()
        hops[k][0].wait_recv()
        on[k][1].start()

    def s2(k):
        to_other[k].wait_recv()
        for c in on[k]:
            c.wait_recv()
        up_out = jnp.dot(gat[k], up_t[...], preferred_element_type=F32)
        hid[k] = jax.nn.gelu(up_out).astype(BF16)
        part = jnp.dot(hid[k], down_v[...], preferred_element_type=F32)
        p_out[k] = part[4 * R :].astype(BF16)
        pair[k].start()
        q_acc[k] = part[: 4 * R]

    def s3(k):
        pair[k].wait_recv()
        for group, c in zip((FAR, LEFT, RIGHT), sums[k]):
            at = pl.ds(R * group, R)
            q_out[k, at] = (q_acc[k, at] + p_in[k, at].astype(F32)).astype(BF16)
            c.start()
        q_acc[k, pl.ds(0, R)] = q_acc[k, pl.ds(0, R)] + p_in[k, pl.ds(0, R)].astype(F32)

    def s4(k):
        for c in sums[k]:
            c.wait_recv()
        r0, r1, r2 = (r_fin[k, n].astype(F32) for n in range(3))
        result = (q_acc[k, pl.ds(0, R)] + r0) + (r1 + r2)
        to_slabs(result, wide_out.at[k], send_d.at[pl.ds(R * k, R)], R)

        def return_row(i, e):
            pltpu.make_async_remote_copy(
                send_d.at[i], recv_d.at[me], a2a_s.at[1], d_r.at[0], device_id=other_core(e), device_id_type=MESH
            ).start()

        for g in range(GPC * k, GPC * (k + 1)):
            each_row(g, lambda i, dy, dz: return_row(i, at_offset(-dy, -dz)))

    stages = (s0, s1, s2, s3, s4)
    order = (0, 1, 10, 2, 20, 11, 30, 3, 21, 31, 12, 22, 40, 13, 32, 23, 41, 33, 42, 43)
    for step in order:
        stages[step // 10](step % 10)

    for c in to_other + pair + sum(hops + on + sums, []):
        c.wait_send()
    slabs_in(send_a, E, a2a_s.at[0])
    slabs_in(send_d, E, a2a_s.at[1])
    slabs_in(recv_d, E, d_r.at[0])
    from_slabs(recv_d, wide, back, E)


def in_hbm(array):
    return pltpu.with_memory_space_constraint(array, pltpu.HBM)


def exchange(images, norm_gain, slot_map, logit_scale, up_weight, down_weight):
    hbm, vmem = pl.BlockSpec(memory_space=pl.ANY), pl.BlockSpec(memory_space=pltpu.VMEM)
    dma = pltpu.SemaphoreType.DMA
    return pl.pallas_call(
        kernel,
        out_shape=(jax.ShapeDtypeStruct((E, D), BF16), jax.ShapeDtypeStruct((TOK, E), BF16)),
        in_specs=[hbm, hbm, hbm, pl.BlockSpec(memory_space=pltpu.SMEM), hbm, hbm],
        out_specs=(vmem, vmem),
        scratch_shapes=[
            pltpu.VMEM((TOK, D), BF16), pltpu.VMEM((D,), BF16), pltpu.VMEM((E, D), BF16),
            pltpu.VMEM((FH, D), BF16), pltpu.VMEM((FH, D), BF16), pltpu.VMEM((D, FH), BF16),
            pltpu.VMEM((TOK, D), BF16), pltpu.VMEM((E, 16, 128), F32),
            pltpu.VMEM((CH, R, 16, 128), F32), pltpu.VMEM((CH, R, 16, 128), F32),
            *[pltpu.VMEM((E, SLAB, 128), BF16)] * 4,
            pltpu.VMEM((CH, 8 * R, D), BF16), pltpu.VMEM((CH, 8 * R, FH), BF16), pltpu.VMEM((CH, 4 * R, D), F32),
            pltpu.VMEM((CH, 4 * R, D), BF16), pltpu.VMEM((CH, 4 * R, D), BF16), pltpu.VMEM((CH, 4 * R, D), BF16),
            pltpu.VMEM((CH, 3, R, D), BF16),
            dma((5,)), dma((2,)), dma((CH,)), dma((1,)), dma((CH, 6)), dma((CH, 6)), dma((CH, 4)), dma((CH, 4)),
        ],
        compiler_params=pltpu.CompilerParams(collective_id=0, has_side_effects=True, vmem_limit_bytes=52 * 1024 * 1024),
    )(in_hbm(images), in_hbm(norm_gain), in_hbm(slot_map.T), logit_scale, in_hbm(up_weight), in_hbm(down_weight))


def local(images, norm_gain, slot_map, logit_scale, up_weight, down_weight):
    back, comb = exchange(images, norm_gain, slot_map, logit_scale, up_weight, down_weight)
    mixed = jnp.einsum("te,ed->td", comb, back, preferred_element_type=F32)
    return (images.astype(F32) + mixed[None]).astype(BF16)


def solution(mesh):
    return jax.shard_map(
        local,
        mesh=mesh,
        in_specs=(
            P(("section", "expert"), None, None),
            P(),
            P(),
            P(),
            P("expert", "section", None),
            P("expert", "section", None),
        ),
        out_specs=P(("section", "expert"), None, None),
        check_vma=False,
    )
```
